128 devices in a mesh: row: 32 (over y, x, core), col: 4 (over z).
Axes of the slice: x: 4, y: 4, z: 4, core: 2. Of those that a mesh axis runs over, the one named last changes fastest.
Arguments:
- velocity: float32 [512, 512, 2048], P(None, 'row', 'col'), may hold values from -6 to 6
- symbol_x: float32 [512], replicated, may hold values from 0.3 to 3
- symbol_y: float32 [512], replicated, may hold values from 0.3 to 3
- symbol_z: float32 [2048], replicated, may hold values from 0.3 to 3
Outputs:
- coefficients: float32 [512, 512, 2048], P('row', 'col')
The draws below stay inside these ranges and needn't reach their ends.
All inputs are finite; a program needn't handle non-finite values.
Results may differ from the reference program's by a relative error of at most 0.000076.
Values sent between devices are 32-bit elements; how exact they have to be, the bound alone decides.
No kernel may reach another device: no remote copies, remote signals or barrier semaphores. Data moves between devices by JAX's collectives and lax.ppermute only.
A program may use at most 192 MiB of HBM per device.

```python
import jax
import jax.numpy as jnp
from jax import lax

GRID_X = 512
GRID_Y = 512
GRID_Z = 2048


def level_of(own_key, shape, pieces, low, largest):
    factor_of = 1.0
    for dim, shards_of in pieces:
        draws = jax.random.uniform(jax.random.fold_in(jax.random.fold_in(own_key, 6), dim), (shards_of,), jnp.float32, low / len(pieces), largest / len(pieces))
        factor_of = factor_of * jnp.repeat(jnp.exp(draws), shape[dim] // shards_of).reshape((-1,) + (1,) * (len(shape) - 1 - dim))
    return factor_of


def normal_values(stream_key, dims, width, limit, split=(), held_as=jnp.bfloat16):
    drawn = jax.random.normal(stream_key, dims, jnp.float32) * width
    if len(split) > 0:
        drawn = level_of(stream_key, dims, split, -0.22, 0.18) * drawn
    return jnp.clip(drawn, min=-limit, max=limit).astype(held_as)


def setup_inputs(seed: int = 0) -> dict:
    seeds = jax.random.split(jax.random.key(seed), 5)
    velocity = normal_values(seeds[0], (GRID_X, GRID_Y, GRID_Z), 1.0, 6.0, ((1, 32), (2, 4)), jnp.float32)
    symbol_x = jnp.clip(jax.random.uniform(seeds[1], (GRID_X,), jnp.float32, 0.3, 3.0), 0.3, 3.0)
    symbol_y = jnp.clip(jax.random.uniform(seeds[2], (GRID_Y,), jnp.float32, 0.3, 3.0), 0.3, 3.0)
    symbol_z = jnp.clip(jax.random.uniform(seeds[3], (GRID_Z,), jnp.float32, 0.3, 3.0), 0.3, 3.0)
    return {"velocity": velocity, "symbol_x": symbol_x, "symbol_y": symbol_y, "symbol_z": symbol_z}


def mode_table(count):
    rank = jnp.arange(count)
    angle = (2.0 * jnp.pi / count) * ((rank[:, None] * rank[None, :]) % count).astype(jnp.float32)
    return (jnp.cos(angle) + jnp.sin(angle)) * (count ** -0.5)


def along_dim(values, dim):
    moved = jnp.tensordot(values, mode_table(values.shape[dim]), axes=([dim], [0]), precision=lax.Precision.HIGHEST)
    return jnp.moveaxis(moved, -1, dim)


def reference(velocity, symbol_x, symbol_y, symbol_z):
    coefficients = velocity
    coefficients = along_dim(coefficients, 0)
    coefficients = along_dim(coefficients, 1)
    coefficients = along_dim(coefficients, 2)
    symbol = symbol_x[:, None, None] + symbol_y[None, :, None] + symbol_z[None, None, :]
    coefficients = coefficients * ((1.0 - 0.2 * symbol) / (1.0 + 0.2 * symbol))
    return coefficients
```

```python
import functools

import jax
import jax.numpy as jnp
import numpy as np
from jax import lax
from jax.experimental import pallas as pl
from jax.experimental.pallas import tpu as pltpu
from jax.sharding import PartitionSpec as P

SIZES = (2, 4, 4, 3, 2, 1)
STARTS = (8, 0, 4, 12, 10, 15)
Z_COLS = 512
VMEM = 60 * 2**20


def halves(x):
    high = x.astype(jnp.bfloat16)
    low = (x - high.astype(jnp.float32)).astype(jnp.bfloat16)
    return high, low


def mm(a, b):
    return lax.dot_general(a, b, (((1,), (0,)), ((), ())), preferred_element_type=jnp.float32)


def mm3(table, x):
    n = table.shape[0] // 2
    high, low = halves(x)
    both = mm(table, high)
    return both[:n] + both[n:] + mm(table[:n], low)


def split_table(table):
    high = lax.reduce_precision(table, 8, 7)
    low = table - high
    return high.astype(jnp.bfloat16), low.astype(jnp.bfloat16)


def stacked(table):
    return jnp.concatenate(split_table(table), axis=0)


def small_table(rank, count):
    turns = (rank[:, None] * jnp.arange(count)[None, :] % count).astype(jnp.float32)
    return jnp.cos(2.0 * jnp.pi / count * turns - jnp.pi / 4) * (2.0 / count) ** 0.5


def x_kernel(ys, group, a_ref, v_ref, *o_refs):
    xs = v_ref.shape[0] // ys
    a = a_ref[...]

    def body(s, _):
        y = s * group
        lines = [v_ref[pl.ds(y + k, xs, stride=ys), :] for k in range(group)]
        out = mm3(a, jnp.concatenate(lines, axis=1))
        first = 0
        for o_ref in o_refs:
            modes = o_ref.shape[0] // ys
            for k in range(group):
                o_ref[pl.ds(y + k, modes, stride=ys), :] = out[first : first + modes, 128 * k : 128 * (k + 1)]
            first += modes
        return 0

    lax.fori_loop(0, ys // group, body, 0)


def x_modes(velocity, table, shares):
    xs, ys, zs = velocity.shape
    modes = table.shape[0] // 2
    flat = velocity.reshape(xs * ys, zs)
    group = 4 if modes < 256 else 2
    return pl.pallas_call(
        functools.partial(x_kernel, ys, group),
        grid=(zs // 128,),
        in_specs=[
            pl.BlockSpec((2 * modes, xs), lambda i: (0, 0)),
            pl.BlockSpec((xs * ys, 128), lambda i: (0, i)),
        ],
        out_specs=[pl.BlockSpec((m * ys, 128), lambda i: (0, i)) for m in shares],
        out_shape=[jax.ShapeDtypeStruct((m * ys, zs), jnp.float32) for m in shares],
        compiler_params=pltpu.CompilerParams(vmem_limit_bytes=VMEM),
        cost_estimate=pl.CostEstimate(flops=6 * modes * xs * ys * zs, bytes_accessed=4 * xs * ys * zs, transcendentals=0),
    )(table, flat)


def y_kernel(a_ref, v_ref, *o_refs):
    blocks, _, ys, width = v_ref.shape
    n = blocks * ys
    out = mm3(a_ref[...], v_ref[...].reshape(n, width))
    share = n // len(o_refs)
    for d, o_ref in enumerate(o_refs):
        o_ref[0] = out[d * share : (d + 1) * share]


def y_modes(values, table, parts):
    blocks, planes, ys, zs = values.shape
    n = blocks * ys
    width = 256
    return pl.pallas_call(
        y_kernel,
        grid=(planes, zs // width),
        in_specs=[
            pl.BlockSpec((2 * n, n), lambda i, k: (0, 0)),
            pl.BlockSpec((blocks, 1, ys, width), lambda i, k: (0, i, 0, k)),
        ],
        out_specs=[pl.BlockSpec((1, n // parts, width), lambda i, k: (i, 0, k))] * parts,
        out_shape=[jax.ShapeDtypeStruct((planes, n // parts, zs), jnp.float32)] * parts,
        compiler_params=pltpu.CompilerParams(vmem_limit_bytes=VMEM),
        cost_estimate=pl.CostEstimate(flops=6 * n * n * zs * planes, bytes_accessed=8 * n * zs * planes, transcendentals=0),
    )(table, values)


def table_kernel(cos_ref, sin_ref, plus_ref, minus_ref, high_ref, low_ref):
    inner = plus_ref.shape[0]
    lines = high_ref.shape[0] // inner
    plus, minus = plus_ref[...], minus_ref[...]
    for k in range(lines):
        i = pl.program_id(0) * lines + k
        cos, sin = cos_ref[pl.ds(i, 1), :], sin_ref[pl.ds(i, 1), :]
        high, low = halves(cos * plus + sin * minus)
        high_ref[k * inner : (k + 1) * inner] = high
        low_ref[k * inner : (k + 1) * inner] = low


def wide_table(outer, inner, count):
    rank = jnp.arange(count)
    unit = 2.0 * jnp.pi / count
    a = unit * (outer[:, None] * rank[None, :] % count).astype(jnp.float32)
    b = unit * (inner[:, None] * rank[None, :] % count).astype(jnp.float32)
    scale = count ** (-0.5)
    cos_b, sin_b = jnp.cos(b), jnp.sin(b)
    lines = pl.BlockSpec((len(outer), count), lambda i: (0, 0))
    whole = pl.BlockSpec((len(inner), count), lambda i: (0, 0))
    block = pl.BlockSpec((4 * len(inner), count), lambda i: (i, 0))
    return pl.pallas_call(
        table_kernel,
        grid=(len(outer) // 4,),
        in_specs=[lines, lines, whole, whole],
        out_specs=[block, block],
        out_shape=[jax.ShapeDtypeStruct((count, count), jnp.bfloat16)] * 2,
        compiler_params=pltpu.CompilerParams(vmem_limit_bytes=VMEM),
        cost_estimate=pl.CostEstimate(flops=10**10, bytes_accessed=4 * count * count, transcendentals=0),
    )(jnp.cos(a) * scale, jnp.sin(a) * scale, cos_b + sin_b, cos_b - sin_b)


def z_kernel(parts, *refs):
    v_refs, (h_ref, l_ref, sxy_ref, sz_ref) = refs[:parts], refs[parts : parts + 4]
    o_ref, high_s, low_s = refs[-3:]
    planes, share, zs = v_refs[0].shape
    rows = planes * share
    pair = pl.program_id(1)

    @pl.when(pl.program_id(0) == 0)
    def _():
        for p, v_ref in enumerate(v_refs):
            high, low = halves(v_ref[...].reshape(rows, zs))
            high_s[pair, :, p * zs : (p + 1) * zs] = high
            low_s[pair, :, p * zs : (p + 1) * zs] = low

    high = high_s[pair]
    hr = h_ref[...]
    out = mm(high, hr) + mm(low_s[pair], hr) + mm(high, l_ref[...])
    sxy = sxy_ref[...]
    for c in range(0, out.shape[1], 128):
        step = 0.2 * (sxy + sz_ref[:, c : c + 128])
        done = out[:, c : c + 128] * ((1.0 - step) / (1.0 + step))
        o_ref[:, :, c : c + 128] = done.reshape(planes, share, 128)


def z_modes(values, tables, sxy, symbol_z, start, total, previous):
    parts = len(values)
    planes, share, zs = values[0].shape
    n = parts * zs
    group = planes
    rows = group * share
    pairs = planes // group
    first = start // group
    assert start % group == 0
    cols = Z_COLS
    operands = [*values, *tables, sxy, symbol_z]
    in_specs = [
        pl.BlockSpec((group, share, zs), lambda i, k: (jnp.where(i == 0, k, pairs - 1), 0, 0))
    ] * parts + [
        pl.BlockSpec((n, cols), lambda i, k: (0, i)),
        pl.BlockSpec((n, cols), lambda i, k: (0, i)),
        pl.BlockSpec((rows, 128), lambda i, k: (first + k, 0)),
        pl.BlockSpec((1, cols), lambda i, k: (0, i)),
    ]
    aliases = {}
    if previous is not None:
        aliases = {len(operands): 0}
        operands.append(previous)
        in_specs.append(pl.BlockSpec(memory_space=pl.ANY))
    return pl.pallas_call(
        functools.partial(z_kernel, parts),
        grid=(n // cols, pairs),
        in_specs=in_specs,
        out_specs=pl.BlockSpec((group, share, cols), lambda i, k: (first + k, 0, i)),
        out_shape=jax.ShapeDtypeStruct((total, share, n), jnp.float32),
        scratch_shapes=[pltpu.VMEM((pairs, rows, n), jnp.bfloat16)] * 2,
        input_output_aliases=aliases,
        compiler_params=pltpu.CompilerParams(vmem_limit_bytes=VMEM),
        cost_estimate=pl.CostEstimate(flops=6 * planes * share * n * n, bytes_accessed=4 * n * n + 8 * planes * share * n, transcendentals=0),
    )(*operands)


def local(velocity, symbol_x, symbol_y, symbol_z):
    xs, ys, zs = velocity.shape
    rows, cols = lax.axis_size("row"), lax.axis_size("col")
    me = lax.axis_index("col")
    planes = xs // rows
    all_y, all_z = ys * rows, zs * cols
    share_y = all_y // cols
    part_x = lax.dynamic_slice_in_dim(symbol_x, lax.axis_index("row") * planes, planes)
    part_y = lax.dynamic_slice_in_dim(symbol_y, me * share_y, share_y)
    sxy = jnp.broadcast_to((part_x[:, None] + part_y[None, :])[..., None], (planes, share_y, 128))
    sxy = sxy.reshape(planes * share_y, 128)
    symbol_z = symbol_z.reshape(1, -1)

    y_rank = (jnp.arange(all_y) + me * share_y) % all_y
    y_table = stacked(small_table(y_rank, all_y))
    low_count = 64
    outer = jnp.arange(all_z // low_count) * low_count
    outer = (me + cols - outer // zs) % cols * zs + outer % zs
    z_tables = wide_table(outer, jnp.arange(low_count), all_z)

    x_parts = []
    for pick in (range(1), range(1, len(SIZES))):
        mode = np.concatenate(
            [(np.arange(rows)[:, None] * planes + STARTS[j] + np.arange(SIZES[j])).reshape(-1) for j in pick]
        )
        x_table = stacked(small_table(jnp.asarray(mode, jnp.int32), xs))
        x_parts += x_modes(velocity, x_table, [rows * SIZES[j] for j in pick])

    out = None
    for j, (size, start) in enumerate(zip(SIZES, STARTS)):
        part = x_parts[j].reshape(rows, size, ys, zs)
        part = lax.all_to_all(part, "row", split_axis=0, concat_axis=0, tiled=True)
        part = y_modes(part, y_table, cols)
        part = [part[0]] + [
            lax.ppermute(part[d], "col", [(i, (i + d) % cols) for i in range(cols)]) for d in range(1, cols)
        ]
        out = z_modes(part, z_tables, sxy, symbol_z, start, planes, out)
    return out


def solution(mesh):
    placed = (P(None, "row", "col"), P(), P(), P())
    return jax.shard_map(local, mesh=mesh, in_specs=placed, out_specs=P("row", "col", None), check_vma=False)
```

```python
import functools

import jax
import jax.numpy as jnp
import numpy as np
from jax import lax
from jax.experimental import pallas as pl
from jax.experimental.pallas import tpu as pltpu
from jax.sharding import PartitionSpec as P

SIZES = (3, 4, 4, 3, 2)
STARTS = (0, 8, 12, 3, 6)
Z_COLS = 512
X_FORM = ((4, 2), (4, 2))
Y_WIDTH = 512
VMEM = 67043328


def halves(x):
    high = x.astype(jnp.bfloat16)
    low = (x - high.astype(jnp.float32)).astype(jnp.bfloat16)
    return high, low


def mm(a, b):
    return lax.dot_general(a, b, (((1,), (0,)), ((), ())), preferred_element_type=jnp.float32)


def mm3(table, x):
    n = table.shape[0] // 2
    high, low = halves(x)
    both = mm(table, high)
    return both[:n] + both[n:] + mm(table[:n], low)


def split_table(table):
    high = lax.reduce_precision(table, 8, 7)
    low = table - high
    return high.astype(jnp.bfloat16), low.astype(jnp.bfloat16)


def stacked(table):
    return jnp.concatenate(split_table(table), axis=0)


def small_table(rank, count):
    turns = (rank[:, None] * jnp.arange(count)[None, :] % count).astype(jnp.float32)
    return jnp.cos(2.0 * jnp.pi / count * turns - jnp.pi / 4) * (2.0 / count) ** 0.5


def x_kernel(group, unroll, a_ref, v_ref, *o_refs):
    xs, _, tile, lanes = v_ref.shape
    v_ref = v_ref.reshape(xs * tile, lanes)
    o_refs = [o_ref.reshape(o_ref.shape[0] * tile, lanes) for o_ref in o_refs]
    a = a_ref[...]

    def body(s, _):
        y = s * group
        lines = [v_ref[pl.ds(y + k, xs, stride=tile), :] for k in range(group)]
        out = mm3(a, jnp.concatenate(lines, axis=1))
        first = 0
        for o_ref in o_refs:
            modes = o_ref.shape[0] // tile
            for k in range(group):
                o_ref[pl.ds(y + k, modes, stride=tile), :] = out[first : first + modes, lanes * k : lanes * (k + 1)]
            first += modes
        return 0

    lax.fori_loop(0, tile // group, body, 0, unroll=unroll)


def x_modes(velocity, table, shares):
    xs, ys, zs = velocity.shape
    modes = table.shape[0] // 2
    tile = 8
    group, unroll = X_FORM[modes < 256]
    return pl.pallas_call(
        functools.partial(x_kernel, group, unroll),
        grid=(zs // 128, ys // tile),
        in_specs=[
            pl.BlockSpec((2 * modes, xs), lambda i, k: (0, 0)),
            pl.BlockSpec((xs, 1, tile, 128), lambda i, k: (0, k, 0, i)),
        ],
        out_specs=[pl.BlockSpec((m, 1, tile, 128), lambda i, k: (0, k, 0, i)) for m in shares],
        out_shape=[jax.ShapeDtypeStruct((m, ys // tile, tile, zs), jnp.float32) for m in shares],
        compiler_params=pltpu.CompilerParams(vmem_limit_bytes=VMEM),
        cost_estimate=pl.CostEstimate(flops=6 * modes * xs * ys * zs, bytes_accessed=4 * xs * ys * zs, transcendentals=0),
    )(table, velocity.reshape(xs, ys // tile, tile, zs))


def y_kernel(a_ref, v_ref, *o_refs):
    blocks, _, ys, width = v_ref.shape
    n = blocks * ys
    out = mm3(a_ref[...], v_ref[...].reshape(n, width))
    share = n // len(o_refs)
    for d, o_ref in enumerate(o_refs):
        o_ref[0] = out[d * share : (d + 1) * share]


def y_modes(values, table, parts):
    blocks, planes, ys, zs = values.shape
    n = blocks * ys
    width = Y_WIDTH
    return pl.pallas_call(
        y_kernel,
        grid=(planes, zs // width),
        in_specs=[
            pl.BlockSpec((2 * n, n), lambda i, k: (0, 0)),
            pl.BlockSpec((blocks, 1, ys, width), lambda i, k: (0, i, 0, k)),
        ],
        out_specs=[pl.BlockSpec((1, n // parts, width), lambda i, k: (i, 0, k))] * parts,
        out_shape=[jax.ShapeDtypeStruct((planes, n // parts, zs), jnp.float32)] * parts,
        compiler_params=pltpu.CompilerParams(vmem_limit_bytes=VMEM),
        cost_estimate=pl.CostEstimate(flops=6 * n * n * zs * planes, bytes_accessed=8 * n * zs * planes, transcendentals=0),
    )(table, values)


def table_kernel(cos_ref, sin_ref, plus_ref, minus_ref, high_ref, low_ref):
    inner = plus_ref.shape[0]
    lines = high_ref.shape[0] // inner
    plus, minus = plus_ref[...], minus_ref[...]
    for k in range(lines):
        i = pl.program_id(0) * lines + k
        cos, sin = cos_ref[pl.ds(i, 1), :], sin_ref[pl.ds(i, 1), :]
        high, low = halves(cos * plus + sin * minus)
        high_ref[k * inner : (k + 1) * inner] = high
        low_ref[k * inner : (k + 1) * inner] = low


def wide_table(outer, inner, count):
    rank = jnp.arange(count)
    unit = 2.0 * jnp.pi / count
    a = unit * (outer[:, None] * rank[None, :] % count).astype(jnp.float32)
    b = unit * (inner[:, None] * rank[None, :] % count).astype(jnp.float32)
    scale = count ** (-0.5)
    cos_b, sin_b = jnp.cos(b), jnp.sin(b)
    lines = pl.BlockSpec((len(outer), count), lambda i: (0, 0))
    whole = pl.BlockSpec((len(inner), count), lambda i: (0, 0))
    block = pl.BlockSpec((4 * len(inner), count), lambda i: (i, 0))
    return pl.pallas_call(
        table_kernel,
        grid=(len(outer) // 4,),
        in_specs=[lines, lines, whole, whole],
        out_specs=[block, block],
        out_shape=[jax.ShapeDtypeStruct((count, count), jnp.bfloat16)] * 2,
        compiler_params=pltpu.CompilerParams(vmem_limit_bytes=VMEM),
        cost_estimate=pl.CostEstimate(flops=10**10, bytes_accessed=4 * count * count, transcendentals=0),
    )(jnp.cos(a) * scale, jnp.sin(a) * scale, cos_b + sin_b, cos_b - sin_b)


def z_kernel(parts, *refs):
    v_refs, (h_ref, l_ref, sxy_ref, sz_ref) = refs[:parts], refs[parts : parts + 4]
    o_ref, high_s, low_s = refs[-3:]
    planes, share, zs = v_refs[0].shape
    rows = planes * share
    pair = pl.program_id(1)

    @pl.when(pl.program_id(0) == 0)
    def _():
        for p, v_ref in enumerate(v_refs):
            high, low = halves(v_ref[...].reshape(rows, zs))
            high_s[pair, :, p * zs : (p + 1) * zs] = high
            low_s[pair, :, p * zs : (p + 1) * zs] = low

    high = high_s[pair]
    hr = h_ref[...]
    out = mm(high, hr) + mm(low_s[pair], hr) + mm(high, l_ref[...])
    sxy = sxy_ref[...]
    for c in range(0, out.shape[1], 128):
        step = 0.2 * (sxy + sz_ref[:, c : c + 128])
        done = out[:, c : c + 128] * ((1.0 - step) / (1.0 + step))
        o_ref[:, :, c : c + 128] = done.reshape(planes, share, 128)


def z_modes(values, tables, sxy, symbol_z, start, total, previous):
    parts = len(values)
    planes, share, zs = values[0].shape
    n = parts * zs
    group = planes
    rows = group * share
    pairs = planes // group
    first = start // group
    assert start % group == 0
    cols = Z_COLS
    operands = [*values, *tables, sxy, symbol_z]
    in_specs = [
        pl.BlockSpec((group, share, zs), lambda i, k: (jnp.where(i == 0, k, pairs - 1), 0, 0))
    ] * parts + [
        pl.BlockSpec((n, cols), lambda i, k: (0, i)),
        pl.BlockSpec((n, cols), lambda i, k: (0, i)),
        pl.BlockSpec((rows, 128), lambda i, k: (first + k, 0)),
        pl.BlockSpec((1, cols), lambda i, k: (0, i)),
    ]
    aliases = {}
    if previous is not None:
        aliases = {len(operands): 0}
        operands.append(previous)
        in_specs.append(pl.BlockSpec(memory_space=pl.ANY))
    return pl.pallas_call(
        functools.partial(z_kernel, parts),
        grid=(n // cols, pairs),
        in_specs=in_specs,
        out_specs=pl.BlockSpec((group, share, cols), lambda i, k: (first + k, 0, i)),
        out_shape=jax.ShapeDtypeStruct((total, share, n), jnp.float32),
        scratch_shapes=[pltpu.VMEM((pairs, rows, n), jnp.bfloat16)] * 2,
        input_output_aliases=aliases,
        compiler_params=pltpu.CompilerParams(vmem_limit_bytes=VMEM),
        cost_estimate=pl.CostEstimate(flops=6 * planes * share * n * n, bytes_accessed=4 * n * n + 8 * planes * share * n, transcendentals=0),
    )(*operands)


def local(velocity, symbol_x, symbol_y, symbol_z):
    xs, ys, zs = velocity.shape
    rows, cols = lax.axis_size("row"), lax.axis_size("col")
    me = lax.axis_index("col")
    planes = xs // rows
    all_y, all_z = ys * rows, zs * cols
    share_y = all_y // cols
    part_x = lax.dynamic_slice_in_dim(symbol_x, lax.axis_index("row") * planes, planes)
    part_y = lax.dynamic_slice_in_dim(symbol_y, me * share_y, share_y)
    sxy = jnp.broadcast_to((part_x[:, None] + part_y[None, :])[..., None], (planes, share_y, 128))
    sxy = sxy.reshape(planes * share_y, 128)
    symbol_z = symbol_z.reshape(1, -1)

    y_rank = (jnp.arange(all_y) + me * share_y) % all_y
    y_table = stacked(small_table(y_rank, all_y))
    low_count = 64
    outer = jnp.arange(all_z // low_count) * low_count
    outer = (me + cols - outer // zs) % cols * zs + outer % zs
    z_tables = wide_table(outer, jnp.arange(low_count), all_z)

    x_parts = []
    for pick in (range(1), range(1, len(SIZES))):
        mode = np.concatenate(
            [(np.arange(rows)[:, None] * planes + STARTS[j] + np.arange(SIZES[j])).reshape(-1) for j in pick]
        )
        x_table = stacked(small_table(jnp.asarray(mode, jnp.int32), xs))
        x_parts += x_modes(velocity, x_table, [rows * SIZES[j] for j in pick])

    out = None
    for j, (size, start) in enumerate(zip(SIZES, STARTS)):
        part = x_parts[j].reshape(rows, size, ys, zs)
        part = lax.all_to_all(part, "row", split_axis=0, concat_axis=0, tiled=True)
        part = y_modes(part, y_table, cols)
        part = [part[0]] + [
            lax.ppermute(part[d], "col", [(i, (i + d) % cols) for i in range(cols)]) for d in range(1, cols)
        ]
        out = z_modes(part, z_tables, sxy, symbol_z, start, planes, out)
    return out


def solution(mesh):
    placed = (P(None, "row", "col"), P(), P(), P())
    return jax.shard_map(local, mesh=mesh, in_specs=placed, out_specs=P("row", "col", None), check_vma=False)
```

```python
import functools

import jax
import jax.numpy as jnp
import numpy as np
from jax import lax
from jax.experimental import pallas as pl
from jax.experimental.pallas import tpu as pltpu
from jax.sharding import PartitionSpec as P

SIZES = (3, 4, 4, 3, 2)
STARTS = (0, 8, 12, 3, 6)
Z_COLS = 512
SPLIT = 2
X_FORM = ((4, 2), (4, 2))
Y_WIDTH = 512
VMEM = 67043328


def halves(x):
    high = x.astype(jnp.bfloat16)
    low = (x - high.astype(jnp.float32)).astype(jnp.bfloat16)
    return high, low


def mm(a, b):
    return lax.dot_general(a, b, (((1,), (0,)), ((), ())), preferred_element_type=jnp.float32)


def mm3(table, x):
    n = table.shape[0] // 2
    high, low = halves(x)
    both = mm(table, high)
    return both[:n] + both[n:] + mm(table[:n], low)


def split_table(table):
    high = lax.reduce_precision(table, 8, 7)
    low = table - high
    return high.astype(jnp.bfloat16), low.astype(jnp.bfloat16)


def stacked(table):
    return jnp.concatenate(split_table(table), axis=0)


def stacked_once(rank, count):
    both = jnp.concatenate([rank, rank])
    table = small_table(both, count)
    high = lax.reduce_precision(table, 8, 7)
    row = lax.broadcasted_iota(jnp.int32, table.shape, 0)
    return jnp.where(row < len(rank), high, table - high).astype(jnp.bfloat16)


def small_table(rank, count):
    turns = (rank[:, None] * jnp.arange(count)[None, :] % count).astype(jnp.float32)
    return jnp.cos(2.0 * jnp.pi / count * turns - jnp.pi / 4) * (2.0 / count) ** 0.5


def x_kernel(group, unroll, a_ref, v_ref, *o_refs):
    xs, _, tile, lanes = v_ref.shape
    v_ref = v_ref.reshape(xs * tile, lanes)
    o_refs = [o_ref.reshape(o_ref.shape[0] * tile, lanes) for o_ref in o_refs]
    a = a_ref[...]

    def body(s, _):
        y = s * group
        lines = [v_ref[pl.ds(y + k, xs, stride=tile), :] for k in range(group)]
        out = mm3(a, jnp.concatenate(lines, axis=1))
        first = 0
        for o_ref in o_refs:
            modes = o_ref.shape[0] // tile
            for k in range(group):
                o_ref[pl.ds(y + k, modes, stride=tile), :] = out[first : first + modes, lanes * k : lanes * (k + 1)]
            first += modes
        return 0

    lax.fori_loop(0, tile // group, body, 0, unroll=unroll)


def x_modes(velocity, table, shares):
    xs, ys, zs = velocity.shape
    modes = table.shape[0] // 2
    tile = 8
    group, unroll = X_FORM[modes < 256]
    return pl.pallas_call(
        functools.partial(x_kernel, group, unroll),
        grid=(zs // 128, ys // tile),
        in_specs=[
            pl.BlockSpec((2 * modes, xs), lambda i, k: (0, 0)),
            pl.BlockSpec((xs, 1, tile, 128), lambda i, k: (0, k, 0, i)),
        ],
        out_specs=[pl.BlockSpec((m, 1, tile, 128), lambda i, k: (0, k, 0, i)) for m in shares],
        out_shape=[jax.ShapeDtypeStruct((m, ys // tile, tile, zs), jnp.float32) for m in shares],
        compiler_params=pltpu.CompilerParams(vmem_limit_bytes=VMEM),
        cost_estimate=pl.CostEstimate(flops=6 * modes * xs * ys * zs, bytes_accessed=4 * xs * ys * zs, transcendentals=0),
    )(table, velocity.reshape(xs, ys // tile, tile, zs))


def y_kernel(a_ref, v_ref, *o_refs):
    blocks, _, ys, width = v_ref.shape
    n = blocks * ys
    out = mm3(a_ref[...], v_ref[...].reshape(n, width))
    share = n // len(o_refs)
    for d, o_ref in enumerate(o_refs):
        o_ref[0] = out[d * share : (d + 1) * share]


def y_modes(values, table, parts):
    blocks, planes, ys, zs = values.shape
    n = blocks * ys
    width = Y_WIDTH
    return pl.pallas_call(
        y_kernel,
        grid=(planes, zs // width),
        in_specs=[
            pl.BlockSpec((2 * n, n), lambda i, k: (0, 0)),
            pl.BlockSpec((blocks, 1, ys, width), lambda i, k: (0, i, 0, k)),
        ],
        out_specs=[pl.BlockSpec((1, n // parts, width), lambda i, k: (i, 0, k))] * parts,
        out_shape=[jax.ShapeDtypeStruct((planes, n // parts, zs), jnp.float32)] * parts,
        compiler_params=pltpu.CompilerParams(vmem_limit_bytes=VMEM),
        cost_estimate=pl.CostEstimate(flops=6 * n * n * zs * planes, bytes_accessed=8 * n * zs * planes, transcendentals=0),
    )(table, values)


def table_kernel(cos_ref, sin_ref, plus_ref, minus_ref, high_ref, low_ref):
    inner = plus_ref.shape[0]
    lines = high_ref.shape[0] // inner
    plus, minus = plus_ref[...], minus_ref[...]
    for k in range(lines):
        i = pl.program_id(0) * lines + k
        cos, sin = cos_ref[pl.ds(i, 1), :], sin_ref[pl.ds(i, 1), :]
        high, low = halves(cos * plus + sin * minus)
        high_ref[k * inner : (k + 1) * inner] = high
        low_ref[k * inner : (k + 1) * inner] = low


def wide_table(outer, inner, count):
    rank = jnp.arange(count)
    unit = 2.0 * jnp.pi / count
    a = unit * (outer[:, None] * rank[None, :] % count).astype(jnp.float32)
    b = unit * (inner[:, None] * rank[None, :] % count).astype(jnp.float32)
    scale = count ** (-0.5)
    cos_b, sin_b = jnp.cos(b), jnp.sin(b)
    lines = pl.BlockSpec((len(outer), count), lambda i: (0, 0))
    whole = pl.BlockSpec((len(inner), count), lambda i: (0, 0))
    block = pl.BlockSpec((4 * len(inner), count), lambda i: (i, 0))
    return pl.pallas_call(
        table_kernel,
        grid=(len(outer) // 4,),
        in_specs=[lines, lines, whole, whole],
        out_specs=[block, block],
        out_shape=[jax.ShapeDtypeStruct((count, count), jnp.bfloat16)] * 2,
        compiler_params=pltpu.CompilerParams(vmem_limit_bytes=VMEM),
        cost_estimate=pl.CostEstimate(flops=10**10, bytes_accessed=4 * count * count, transcendentals=0),
    )(jnp.cos(a) * scale, jnp.sin(a) * scale, cos_b + sin_b, cos_b - sin_b)


def z_kernel(parts, summed, final, *refs):
    v_refs, (h_ref, l_ref, sxy_ref, sz_ref) = refs[:parts], refs[parts : parts + 4]
    sum_ref = refs[parts + 4] if summed else None
    o_ref, high_s, low_s = refs[-3:]
    planes, share, zs = v_refs[0].shape
    rows = planes * share

    @pl.when(pl.program_id(0) == 0)
    def _():
        for p, v_ref in enumerate(v_refs):
            high, low = halves(v_ref[...].reshape(rows, zs))
            high_s[:, p * zs : (p + 1) * zs] = high
            low_s[:, p * zs : (p + 1) * zs] = low

    high = high_s[...]
    hr = h_ref[...]
    out = mm(high, hr) + mm(low_s[...], hr) + mm(high, l_ref[...])
    cols = out.shape[1]
    if summed:
        out = out + sum_ref[...].reshape(rows, cols)
    if not final:
        o_ref[...] = out.reshape(planes, share, cols)
        return
    sxy = sxy_ref[...]
    for c in range(0, cols, 128):
        step = 0.2 * (sxy + sz_ref[:, c : c + 128])
        done = out[:, c : c + 128] * ((1.0 - step) / (1.0 + step))
        o_ref[:, :, c : c + 128] = done.reshape(planes, share, 128)


def z_modes(values, part, tables, sxy, symbol_z, start, total, previous, summed=None, final=True):
    planes, share, zs = values[0].shape
    depth = len(values) * zs
    n = tables[0].shape[0]
    rows = planes * share
    first = start // planes
    assert start % planes == 0 and part % len(values) == 0
    block = part // len(values)
    cols = Z_COLS
    operands = [*values, *tables, sxy, symbol_z]
    in_specs = [pl.BlockSpec((planes, share, zs), lambda i: (0, 0, 0))] * len(values) + [
        pl.BlockSpec((depth, cols), lambda i: (block, i)),
        pl.BlockSpec((depth, cols), lambda i: (block, i)),
        pl.BlockSpec((rows, 128), lambda i: (first, 0)),
        pl.BlockSpec((1, cols), lambda i: (0, i)),
    ]
    if summed is not None:
        operands.append(summed)
        in_specs.append(pl.BlockSpec((planes, share, cols), lambda i: (0, 0, i)))
    aliases = {}
    if final and previous is not None:
        aliases = {len(operands): 0}
        operands.append(previous)
        in_specs.append(pl.BlockSpec(memory_space=pl.ANY))
    place = first if final else 0
    return pl.pallas_call(
        functools.partial(z_kernel, len(values), summed is not None, final),
        grid=(n // cols,),
        in_specs=in_specs,
        out_specs=pl.BlockSpec((planes, share, cols), lambda i: (place, 0, i)),
        out_shape=jax.ShapeDtypeStruct((total if final else planes, share, n), jnp.float32),
        scratch_shapes=[pltpu.VMEM((rows, depth), jnp.bfloat16)] * 2,
        input_output_aliases=aliases,
        compiler_params=pltpu.CompilerParams(vmem_limit_bytes=VMEM),
        cost_estimate=pl.CostEstimate(flops=6 * rows * depth * n, bytes_accessed=4 * depth * n + 8 * rows * n, transcendentals=0),
    )(*operands)


def local(velocity, symbol_x, symbol_y, symbol_z):
    xs, ys, zs = velocity.shape
    rows, cols = lax.axis_size("row"), lax.axis_size("col")
    me = lax.axis_index("col")
    planes = xs // rows
    all_y, all_z = ys * rows, zs * cols
    share_y = all_y // cols
    part_x = lax.dynamic_slice_in_dim(symbol_x, lax.axis_index("row") * planes, planes)
    part_y = lax.dynamic_slice_in_dim(symbol_y, me * share_y, share_y)
    sxy = jnp.broadcast_to((part_x[:, None] + part_y[None, :])[..., None], (planes, share_y, 128))
    sxy = sxy.reshape(planes * share_y, 128)
    symbol_z = symbol_z.reshape(1, -1)

    y_rank = (jnp.arange(all_y) + me * share_y) % all_y
    y_table = stacked(small_table(y_rank, all_y))
    low_count = 64
    outer = jnp.arange(all_z // low_count) * low_count
    hop = outer // zs
    hop = jnp.where(hop < 2, hop, 5 - hop)
    outer = (me + cols - hop) % cols * zs + outer % zs
    z_tables = wide_table(outer, jnp.arange(low_count), all_z)

    x_parts = []
    for name, pick in (("x0", range(1)), ("x1", range(1, len(SIZES)))):
        mode = np.concatenate(
            [(np.arange(rows)[:, None] * planes + STARTS[j] + np.arange(SIZES[j])).reshape(-1) for j in pick]
        )
        mode = jnp.asarray(mode, jnp.int32)
        x_table = stacked_once(mode, xs) if name == "x0" else stacked(small_table(mode, xs))
        x_parts += x_modes(velocity, x_table, [rows * SIZES[j] for j in pick])

    out = None
    for j, (size, start) in enumerate(zip(SIZES, STARTS)):
        part = x_parts[j].reshape(rows, size, ys, zs)
        part = lax.all_to_all(part, "row", split_axis=0, concat_axis=0, tiled=True)
        part = y_modes(part, y_table, cols)
        moved = [part[0]]
        for d in (1, 3, 2):
            moved.append(lax.ppermute(part[d], "col", [(i, (i + d) % cols) for i in range(cols)]))
        rest = (z_tables, sxy, symbol_z, start, planes, out)
        if j < len(SIZES) - SPLIT:
            out = z_modes(moved, 0, *rest)
        else:
            early = z_modes(moved[:3], 0, *rest, final=False)
            out = z_modes(moved[3:], 3, *rest, summed=early)
    return out


def solution(mesh):
    placed = (P(None, "row", "col"), P(), P(), P())
    return jax.shard_map(local, mesh=mesh, in_specs=placed, out_specs=P("row", "col", None), check_vma=False)
```

```python
import functools

import jax
import jax.numpy as jnp
import numpy as np
from jax import lax
from jax.experimental import pallas as pl
from jax.experimental.pallas import tpu as pltpu
from jax.sharding import PartitionSpec as P

SIZES = (5, 4, 3, 2, 2)
STARTS = (0, 5, 9, 12, 14)
Z_COLS = 512
X_FORM = ((4, 2), (4, 2))
Y_WIDTH = 512
VMEM = 67043328


def halves(x):
    high = x.astype(jnp.bfloat16)
    low = (x - high.astype(jnp.float32)).astype(jnp.bfloat16)
    return high, low


def mm(a, b):
    return lax.dot_general(a, b, (((1,), (0,)), ((), ())), preferred_element_type=jnp.float32)


def mm3(table, x):
    n = table.shape[0] // 2
    high, low = halves(x)
    both = mm(table, high)
    return both[:n] + both[n:] + mm(table[:n], low)


def split_table(table):
    high = lax.reduce_precision(table, 8, 7)
    low = table - high
    return high.astype(jnp.bfloat16), low.astype(jnp.bfloat16)


def stacked(table):
    return jnp.concatenate(split_table(table), axis=0)


def fixed_table(rank, count):
    turns = rank[:, None] * np.arange(count)[None, :] % count
    table = np.cos(2.0 * np.pi / count * turns - np.pi / 4) * (2.0 / count) ** 0.5
    high = table.astype(jnp.bfloat16)
    low = (table - high.astype(np.float64)).astype(jnp.bfloat16)
    return jnp.asarray(np.concatenate([high, low]))


def small_table(rank, count):
    turns = (rank[:, None] * jnp.arange(count)[None, :] % count).astype(jnp.float32)
    return jnp.cos(2.0 * jnp.pi / count * turns - jnp.pi / 4) * (2.0 / count) ** 0.5


def x_kernel(group, unroll, a_ref, v_ref, *o_refs):
    xs, _, tile, lanes = v_ref.shape
    v_ref = v_ref.reshape(xs * tile, lanes)
    o_refs = [o_ref.reshape(o_ref.shape[0] * tile, lanes) for o_ref in o_refs]
    a = a_ref[...]

    def body(s, _):
        y = s * group
        lines = [v_ref[pl.ds(y + k, xs, stride=tile), :] for k in range(group)]
        out = mm3(a, jnp.concatenate(lines, axis=1))
        first = 0
        for o_ref in o_refs:
            modes = o_ref.shape[0] // tile
            for k in range(group):
                o_ref[pl.ds(y + k, modes, stride=tile), :] = out[first : first + modes, lanes * k : lanes * (k + 1)]
            first += modes
        return 0

    lax.fori_loop(0, tile // group, body, 0, unroll=unroll)


def x_modes(velocity, table, shares):
    xs, ys, zs = velocity.shape
    modes = table.shape[0] // 2
    tile = 8
    group, unroll = X_FORM[modes < 256]
    return pl.pallas_call(
        functools.partial(x_kernel, group, unroll),
        grid=(zs // 128, ys // tile),
        in_specs=[
            pl.BlockSpec((2 * modes, xs), lambda i, k: (0, 0)),
            pl.BlockSpec((xs, 1, tile, 128), lambda i, k: (0, k, 0, i)),
        ],
        out_specs=[pl.BlockSpec((m, 1, tile, 128), lambda i, k: (0, k, 0, i)) for m in shares],
        out_shape=[jax.ShapeDtypeStruct((m, ys // tile, tile, zs), jnp.float32) for m in shares],
        compiler_params=pltpu.CompilerParams(vmem_limit_bytes=VMEM),
        cost_estimate=pl.CostEstimate(flops=6 * modes * xs * ys * zs, bytes_accessed=4 * xs * ys * zs, transcendentals=0),
    )(table, velocity.reshape(xs, ys // tile, tile, zs))


def y_kernel(a_ref, v_ref, *o_refs):
    blocks, _, ys, width = v_ref.shape
    n = blocks * ys
    out = mm3(a_ref[...], v_ref[...].reshape(n, width))
    share = n // len(o_refs)
    for d, o_ref in enumerate(o_refs):
        o_ref[0] = out[d * share : (d + 1) * share]


def y_modes(values, table, parts):
    blocks, planes, ys, zs = values.shape
    n = blocks * ys
    width = Y_WIDTH
    return pl.pallas_call(
        y_kernel,
        grid=(planes, zs // width),
        in_specs=[
            pl.BlockSpec((2 * n, n), lambda i, k: (0, 0)),
            pl.BlockSpec((blocks, 1, ys, width), lambda i, k: (0, i, 0, k)),
        ],
        out_specs=[pl.BlockSpec((1, n // parts, width), lambda i, k: (i, 0, k))] * parts,
        out_shape=[jax.ShapeDtypeStruct((planes, n // parts, zs), jnp.float32)] * parts,
        compiler_params=pltpu.CompilerParams(vmem_limit_bytes=VMEM),
        cost_estimate=pl.CostEstimate(flops=6 * n * n * zs * planes, bytes_accessed=8 * n * zs * planes, transcendentals=0),
    )(table, values)


def table_kernel(cos_ref, sin_ref, plus_ref, minus_ref, high_ref, low_ref):
    inner = plus_ref.shape[0]
    lines = high_ref.shape[0] // inner
    plus, minus = plus_ref[...], minus_ref[...]
    for k in range(lines):
        i = pl.program_id(0) * lines + k
        cos, sin = cos_ref[pl.ds(i, 1), :], sin_ref[pl.ds(i, 1), :]
        high, low = halves(cos * plus + sin * minus)
        high_ref[k * inner : (k + 1) * inner] = high
        low_ref[k * inner : (k + 1) * inner] = low


def wide_table(outer, inner, count):
    rank = jnp.arange(count)
    unit = 2.0 * jnp.pi / count
    a = unit * (outer[:, None] * rank[None, :] % count).astype(jnp.float32)
    b = unit * (inner[:, None] * rank[None, :] % count).astype(jnp.float32)
    scale = count ** (-0.5)
    cos_b, sin_b = jnp.cos(b), jnp.sin(b)
    lines = pl.BlockSpec((len(outer), count), lambda i: (0, 0))
    whole = pl.BlockSpec((len(inner), count), lambda i: (0, 0))
    block = pl.BlockSpec((4 * len(inner), count), lambda i: (i, 0))
    return pl.pallas_call(
        table_kernel,
        grid=(len(outer) // 4,),
        in_specs=[lines, lines, whole, whole],
        out_specs=[block, block],
        out_shape=[jax.ShapeDtypeStruct((count, count), jnp.bfloat16)] * 2,
        compiler_params=pltpu.CompilerParams(vmem_limit_bytes=VMEM),
        cost_estimate=pl.CostEstimate(flops=10**10, bytes_accessed=4 * count * count, transcendentals=0),
    )(jnp.cos(a) * scale, jnp.sin(a) * scale, cos_b + sin_b, cos_b - sin_b)


def z_kernel(parts, *refs):
    v_refs, (h_ref, l_ref, sxy_ref, sz_ref) = refs[:parts], refs[parts : parts + 4]
    o_ref, high_s, low_s = refs[-3:]
    planes, share, zs = v_refs[0].shape
    rows = planes * share
    pair = pl.program_id(1)

    @pl.when(pl.program_id(0) == 0)
    def _():
        for p, v_ref in enumerate(v_refs):
            high, low = halves(v_ref[...].reshape(rows, zs))
            high_s[pair, :, p * zs : (p + 1) * zs] = high
            low_s[pair, :, p * zs : (p + 1) * zs] = low

    high = high_s[pair]
    hr = h_ref[...]
    out = mm(high, hr) + mm(low_s[pair], hr) + mm(high, l_ref[...])
    sxy = sxy_ref[...]
    for c in range(0, out.shape[1], 128):
        step = 0.2 * (sxy + sz_ref[:, c : c + 128])
        done = out[:, c : c + 128] * ((1.0 - step) / (1.0 + step))
        o_ref[:, :, c : c + 128] = done.reshape(planes, share, 128)


def z_modes(values, tables, sxy, symbol_z, start, total, previous):
    parts = len(values)
    planes, share, zs = values[0].shape
    n = parts * zs
    group = planes
    rows = group * share
    pairs = planes // group
    cols = Z_COLS
    operands = [*values, *tables, sxy, symbol_z]
    in_specs = [
        pl.BlockSpec((group, share, zs), lambda i, k: (jnp.where(i == 0, k, pairs - 1), 0, 0))
    ] * parts + [
        pl.BlockSpec((n, cols), lambda i, k: (0, i)),
        pl.BlockSpec((n, cols), lambda i, k: (0, i)),
        pl.BlockSpec((pl.Element(rows), pl.Element(128)), lambda i, k: (start * share, 0)),
        pl.BlockSpec((1, cols), lambda i, k: (0, i)),
    ]
    aliases = {}
    if previous is not None:
        aliases = {len(operands): 0}
        operands.append(previous)
        in_specs.append(pl.BlockSpec(memory_space=pl.ANY))
    return pl.pallas_call(
        functools.partial(z_kernel, parts),
        grid=(n // cols, pairs),
        in_specs=in_specs,
        out_specs=pl.BlockSpec(
            (pl.Element(group), pl.Element(share), pl.Element(cols)), lambda i, k: (start, 0, i * cols)
        ),
        out_shape=jax.ShapeDtypeStruct((total, share, n), jnp.float32),
        scratch_shapes=[pltpu.VMEM((pairs, rows, n), jnp.bfloat16)] * 2,
        input_output_aliases=aliases,
        compiler_params=pltpu.CompilerParams(vmem_limit_bytes=VMEM),
        cost_estimate=pl.CostEstimate(flops=6 * planes * share * n * n, bytes_accessed=4 * n * n + 8 * planes * share * n, transcendentals=0),
    )(*operands)


def local(velocity, symbol_x, symbol_y, symbol_z):
    xs, ys, zs = velocity.shape
    rows, cols = lax.axis_size("row"), lax.axis_size("col")
    me = lax.axis_index("col")
    planes = xs // rows
    all_y, all_z = ys * rows, zs * cols
    share_y = all_y // cols
    part_x = lax.dynamic_slice_in_dim(symbol_x, lax.axis_index("row") * planes, planes)
    part_y = lax.dynamic_slice_in_dim(symbol_y, me * share_y, share_y)
    sxy = jnp.broadcast_to((part_x[:, None] + part_y[None, :])[..., None], (planes, share_y, 128))
    sxy = sxy.reshape(planes * share_y, 128)
    symbol_z = symbol_z.reshape(1, -1)

    y_rank = (jnp.arange(all_y) + me * share_y) % all_y
    y_table = stacked(small_table(y_rank, all_y))
    low_count = 64
    outer = jnp.arange(all_z // low_count) * low_count
    outer = (me + cols - outer // zs) % cols * zs + outer % zs
    z_tables = wide_table(outer, jnp.arange(low_count), all_z)

    x_parts = []
    for name, pick in (("x0", range(1)), ("x1", range(1, len(SIZES)))):
        mode = np.concatenate(
            [(np.arange(rows)[:, None] * planes + STARTS[j] + np.arange(SIZES[j])).reshape(-1) for j in pick]
        )
        if name == "x0":
            x_table = fixed_table(mode, xs)
        else:
            x_table = stacked(small_table(jnp.asarray(mode, jnp.int32), xs))
        x_parts += x_modes(velocity, x_table, [rows * SIZES[j] for j in pick])

    out = None
    for j, (size, start) in enumerate(zip(SIZES, STARTS)):
        part = x_parts[j].reshape(rows, size, ys, zs)
        part = lax.all_to_all(part, "row", split_axis=0, concat_axis=0, tiled=True)
        part = y_modes(part, y_table, cols)
        part = [part[0]] + [
            lax.ppermute(part[d], "col", [(i, (i + d) % cols) for i in range(cols)]) for d in range(1, cols)
        ]
        out = z_modes(part, z_tables, sxy, symbol_z, start, planes, out)
    return out


def solution(mesh):
    placed = (P(None, "row", "col"), P(), P(), P())
    return jax.shard_map(local, mesh=mesh, in_specs=placed, out_specs=P("row", "col", None), check_vma=False)
```

```python
import functools

import jax
import jax.numpy as jnp
import numpy as np
from jax import lax
from jax.experimental import pallas as pl
from jax.experimental.pallas import tpu as pltpu
from jax.sharding import PartitionSpec as P

SIZES = (5, 4, 3, 2, 2)
STARTS = (0, 5, 9, 12, 14)
Z_COLS = 512
X_FORM = ((4, 2), (4, 2))
Y_WIDTH = 512
VMEM = 67043328


def halves(x):
    high = x.astype(jnp.bfloat16)
    low = (x - high.astype(jnp.float32)).astype(jnp.bfloat16)
    return high, low


def mm(a, b):
    return lax.dot_general(a, b, (((1,), (0,)), ((), ())), preferred_element_type=jnp.float32)


def mm3(table, x):
    n = table.shape[0] // 2
    high, low = halves(x)
    both = mm(table, high)
    return both[:n] + both[n:] + mm(table[:n], low)


def split_table(table):
    high = lax.reduce_precision(table, 8, 7)
    low = table - high
    return high.astype(jnp.bfloat16), low.astype(jnp.bfloat16)


def stacked(table):
    return jnp.concatenate(split_table(table), axis=0)


def fixed_table(rank, count):
    turns = rank[:, None] * np.arange(count)[None, :] % count
    table = np.cos(2.0 * np.pi / count * turns - np.pi / 4) * (2.0 / count) ** 0.5
    high = table.astype(jnp.bfloat16)
    low = (table - high.astype(np.float64)).astype(jnp.bfloat16)
    return jnp.asarray(np.concatenate([high, low]))


def small_table(rank, count):
    turns = (rank[:, None] * jnp.arange(count)[None, :] % count).astype(jnp.float32)
    return jnp.cos(2.0 * jnp.pi / count * turns - jnp.pi / 4) * (2.0 / count) ** 0.5


def x_kernel(group, unroll, a_ref, v_ref, *o_refs):
    xs, _, tile, lanes = v_ref.shape
    v_ref = v_ref.reshape(xs * tile, lanes)
    o_refs = [o_ref.reshape(o_ref.shape[0] * tile, lanes) for o_ref in o_refs]
    a = a_ref[...]

    def body(s, _):
        y = s * group
        lines = [v_ref[pl.ds(y + k, xs, stride=tile), :] for k in range(group)]
        out = mm3(a, jnp.concatenate(lines, axis=1))
        first = 0
        for o_ref in o_refs:
            modes = o_ref.shape[0] // tile
            for k in range(group):
                o_ref[pl.ds(y + k, modes, stride=tile), :] = out[first : first + modes, lanes * k : lanes * (k + 1)]
            first += modes
        return 0

    lax.fori_loop(0, tile // group, body, 0, unroll=unroll)


def x_modes(velocity, table, shares):
    xs, ys, zs = velocity.shape
    modes = table.shape[0] // 2
    tile = 8
    group, unroll = X_FORM[modes < 256]
    return pl.pallas_call(
        functools.partial(x_kernel, group, unroll),
        grid=(zs // 128, ys // tile),
        in_specs=[
            pl.BlockSpec((2 * modes, xs), lambda i, k: (0, 0)),
            pl.BlockSpec((xs, 1, tile, 128), lambda i, k: (0, k, 0, i)),
        ],
        out_specs=[pl.BlockSpec((m, 1, tile, 128), lambda i, k: (0, k, 0, i)) for m in shares],
        out_shape=[jax.ShapeDtypeStruct((m, ys // tile, tile, zs), jnp.float32) for m in shares],
        compiler_params=pltpu.CompilerParams(vmem_limit_bytes=VMEM),
        cost_estimate=pl.CostEstimate(flops=6 * modes * xs * ys * zs, bytes_accessed=4 * xs * ys * zs, transcendentals=0),
    )(table, velocity.reshape(xs, ys // tile, tile, zs))


def y_kernel(a_ref, v_ref, *o_refs):
    blocks, _, ys, width = v_ref.shape
    n = blocks * ys
    out = mm3(a_ref[...], v_ref[...].reshape(n, width))
    share = n // len(o_refs)
    for d, o_ref in enumerate(o_refs):
        o_ref[0] = out[d * share : (d + 1) * share]


def y_modes(values, table, parts):
    blocks, planes, ys, zs = values.shape
    n = blocks * ys
    width = Y_WIDTH
    return pl.pallas_call(
        y_kernel,
        grid=(planes, zs // width),
        in_specs=[
            pl.BlockSpec((2 * n, n), lambda i, k: (0, 0)),
            pl.BlockSpec((blocks, 1, ys, width), lambda i, k: (0, i, 0, k)),
        ],
        out_specs=[pl.BlockSpec((1, n // parts, width), lambda i, k: (i, 0, k))] * parts,
        out_shape=[jax.ShapeDtypeStruct((planes, n // parts, zs), jnp.float32)] * parts,
        compiler_params=pltpu.CompilerParams(vmem_limit_bytes=VMEM),
        cost_estimate=pl.CostEstimate(flops=6 * n * n * zs * planes, bytes_accessed=8 * n * zs * planes, transcendentals=0),
    )(table, values)


def table_kernel(cos_ref, sin_ref, plus_ref, minus_ref, high_ref, low_ref):
    inner = plus_ref.shape[0]
    lines = high_ref.shape[0] // inner
    plus, minus = plus_ref[...], minus_ref[...]
    for k in range(lines):
        i = pl.program_id(0) * lines + k
        cos, sin = cos_ref[pl.ds(i, 1), :], sin_ref[pl.ds(i, 1), :]
        high, low = halves(cos * plus + sin * minus)
        high_ref[k * inner : (k + 1) * inner] = high
        low_ref[k * inner : (k + 1) * inner] = low


def wide_table(outer, inner, rank, count):
    width = len(rank)
    unit = 2.0 * jnp.pi / count
    a = unit * (outer[:, None] * rank[None, :] % count).astype(jnp.float32)
    b = unit * (inner[:, None] * rank[None, :] % count).astype(jnp.float32)
    scale = count ** (-0.5)
    cos_b, sin_b = jnp.cos(b), jnp.sin(b)
    lines = pl.BlockSpec((len(outer), width), lambda i: (0, 0))
    whole = pl.BlockSpec((len(inner), width), lambda i: (0, 0))
    block = pl.BlockSpec((4 * len(inner), width), lambda i: (i, 0))
    shape = jax.ShapeDtypeStruct((len(outer) * len(inner), width), jnp.bfloat16)
    return pl.pallas_call(
        table_kernel,
        grid=(len(outer) // 4,),
        in_specs=[lines, lines, whole, whole],
        out_specs=[block, block],
        out_shape=[shape, shape],
        compiler_params=pltpu.CompilerParams(vmem_limit_bytes=VMEM),
        cost_estimate=pl.CostEstimate(flops=10**10, bytes_accessed=2 * count * count, transcendentals=0),
    )(jnp.cos(a) * scale, jnp.sin(a) * scale, cos_b + sin_b, cos_b - sin_b)


def z_kernel(parts, *refs):
    v_refs = refs[:parts]
    he_ref, ho_ref, le_ref, lo_ref, sxy_ref, sz_ref = refs[parts : parts + 6]
    o_ref, high_s, low_s = refs[-3:]
    planes, share, zs = v_refs[0].shape
    rows = planes * share

    @pl.when(pl.program_id(0) == 0)
    def _():
        for p in range(parts // 2):
            near, far = v_refs[p][...].reshape(rows, zs), v_refs[p + parts // 2][...].reshape(rows, zs)
            for k, mixed in enumerate((near + far, near - far)):
                high, low = halves(mixed)
                high_s[k, :, p * zs : (p + 1) * zs] = high
                low_s[k, :, p * zs : (p + 1) * zs] = low

    both = []
    for k, (h_ref, l_ref) in enumerate(((he_ref, le_ref), (ho_ref, lo_ref))):
        high, hr = high_s[k], h_ref[...]
        both.append(mm(high, hr) + mm(low_s[k], hr) + mm(high, l_ref[...]))
    even, odd = both
    sxy = sxy_ref[...]
    lane = lax.broadcasted_iota(jnp.int32, (rows, 128), 1)
    for c in range(0, o_ref.shape[2], 128):
        g = c // 256 * 128
        pick = lane // 2 + c // 128 % 2 * 64
        here = [jnp.take_along_axis(t[:, g : g + 128], pick, axis=1, mode="promise_in_bounds") for t in (even, odd)]
        out = jnp.where(lane % 2 == 0, *here)
        step = 0.2 * (sxy + sz_ref[:, c : c + 128])
        done = out * ((1.0 - step) / (1.0 + step))
        o_ref[:, :, c : c + 128] = done.reshape(planes, share, 128)


def z_modes(values, tables, sxy, symbol_z, start, total, previous):
    parts = len(values)
    planes, share, zs = values[0].shape
    n = parts * zs
    rows = planes * share
    cols = Z_COLS
    steps = n // cols
    high, low = tables
    table_specs = [
        pl.BlockSpec((n // 2, cols // 2), lambda i: (0, i)),
        pl.BlockSpec((n // 2, cols // 2), lambda i: (0, steps + i)),
    ]
    operands = [*values, high, high, low, low, sxy, symbol_z]
    in_specs = [pl.BlockSpec((planes, share, zs), lambda i: (0, 0, 0))] * parts + table_specs * 2 + [
        pl.BlockSpec((pl.Element(rows), pl.Element(128)), lambda i: (start * share, 0)),
        pl.BlockSpec((1, cols), lambda i: (0, i)),
    ]
    aliases = {}
    if previous is not None:
        aliases = {len(operands): 0}
        operands.append(previous)
        in_specs.append(pl.BlockSpec(memory_space=pl.ANY))
    return pl.pallas_call(
        functools.partial(z_kernel, parts),
        grid=(steps,),
        in_specs=in_specs,
        out_specs=pl.BlockSpec(
            (pl.Element(planes), pl.Element(share), pl.Element(cols)), lambda i: (start, 0, i * cols)
        ),
        out_shape=jax.ShapeDtypeStruct((total, share, n), jnp.float32),
        scratch_shapes=[pltpu.VMEM((2, rows, n // 2), jnp.bfloat16)] * 2,
        input_output_aliases=aliases,
        compiler_params=pltpu.CompilerParams(vmem_limit_bytes=VMEM),
        cost_estimate=pl.CostEstimate(flops=3 * rows * n * n, bytes_accessed=2 * n * n + 8 * rows * n, transcendentals=0),
    )(*operands)


def local(velocity, symbol_x, symbol_y, symbol_z):
    xs, ys, zs = velocity.shape
    rows, cols = lax.axis_size("row"), lax.axis_size("col")
    me = lax.axis_index("col")
    planes = xs // rows
    all_y, all_z = ys * rows, zs * cols
    share_y = all_y // cols
    part_x = lax.dynamic_slice_in_dim(symbol_x, lax.axis_index("row") * planes, planes)
    part_y = lax.dynamic_slice_in_dim(symbol_y, me * share_y, share_y)
    sxy = jnp.broadcast_to((part_x[:, None] + part_y[None, :])[..., None], (planes, share_y, 128))
    sxy = sxy.reshape(planes * share_y, 128)
    symbol_z = symbol_z.reshape(1, -1)

    y_rank = (jnp.arange(all_y) + me * share_y) % all_y
    y_table = stacked(small_table(y_rank, all_y))
    low_count = 64
    outer = jnp.arange(all_z // 2 // low_count) * low_count
    outer = (me + cols - outer // zs) % cols * zs + outer % zs
    lane = jnp.arange(all_z)
    half = all_z // 2
    z_tables = wide_table(outer, jnp.arange(low_count), lane % half * 2 + lane // half, all_z)

    x_parts = []
    for name, pick in (("x0", range(1)), ("x1", range(1, len(SIZES)))):
        mode = np.concatenate(
            [(np.arange(rows)[:, None] * planes + STARTS[j] + np.arange(SIZES[j])).reshape(-1) for j in pick]
        )
        if name == "x0":
            x_table = fixed_table(mode, xs)
        else:
            x_table = stacked(small_table(jnp.asarray(mode, jnp.int32), xs))
        x_parts += x_modes(velocity, x_table, [rows * SIZES[j] for j in pick])

    out = None
    for j, (size, start) in enumerate(zip(SIZES, STARTS)):
        part = x_parts[j].reshape(rows, size, ys, zs)
        part = lax.all_to_all(part, "row", split_axis=0, concat_axis=0, tiled=True)
        part = y_modes(part, y_table, cols)
        part = [part[0]] + [
            lax.ppermute(part[d], "col", [(i, (i + d) % cols) for i in range(cols)]) for d in range(1, cols)
        ]
        out = z_modes(part, z_tables, sxy, symbol_z, start, planes, out)
    return out


def solution(mesh):
    placed = (P(None, "row", "col"), P(), P(), P())
    return jax.shard_map(local, mesh=mesh, in_specs=placed, out_specs=P("row", "col", None), check_vma=False)
```

```python
import functools

import jax
import jax.numpy as jnp
import numpy as np
from jax import lax
from jax.experimental import pallas as pl
from jax.experimental.pallas import tpu as pltpu
from jax.sharding import PartitionSpec as P

CHUNKS = ((0, 8, 0, 2), (0, 8, 1, 2), (8, 4, 0, 1), (12, 3, 0, 1), (15, 1, 0, 1))
Z_COLS = 512
VMEM = 67043328


def halves(x):
    high = x.astype(jnp.bfloat16)
    low = (x - high.astype(jnp.float32)).astype(jnp.bfloat16)
    return high, low


def mm(a, b):
    return lax.dot_general(a, b, (((1,), (0,)), ((), ())), preferred_element_type=jnp.float32)


def mm3(table, x):
    n = table.shape[0] // 2
    high, low = halves(x)
    both = mm(table, high)
    return both[:n] + both[n:] + mm(table[:n], low)


def split_table(table):
    high = lax.reduce_precision(table, 8, 7)
    low = table - high
    return high.astype(jnp.bfloat16), low.astype(jnp.bfloat16)


def stacked(table):
    return jnp.concatenate(split_table(table), axis=0)


def fixed_table(rank, count):
    turns = rank[:, None] * np.arange(count)[None, :] % count
    table = np.cos(2.0 * np.pi / count * turns - np.pi / 4) * (2.0 / count) ** 0.5
    high = table.astype(jnp.bfloat16)
    low = (table - high.astype(np.float64)).astype(jnp.bfloat16)
    return jnp.asarray(np.concatenate([high, low]))


def small_table(rank, count):
    turns = (rank[:, None] * jnp.arange(count)[None, :] % count).astype(jnp.float32)
    return jnp.cos(2.0 * jnp.pi / count * turns - jnp.pi / 4) * (2.0 / count) ** 0.5


def x_kernel(a_ref, v_ref, *o_refs):
    xs, _, tile, lanes = v_ref.shape
    v_ref = v_ref.reshape(xs * tile, lanes)
    o_refs = [o_ref.reshape(o_ref.shape[0] * tile, lanes) for o_ref in o_refs]
    a = a_ref[...]

    def body(s, _):
        y = s * 4
        lines = [v_ref[pl.ds(y + k, xs, stride=tile), :] for k in range(4)]
        out = mm3(a, jnp.concatenate(lines, axis=1))
        first = 0
        for o_ref in o_refs:
            modes = o_ref.shape[0] // tile
            for k in range(4):
                o_ref[pl.ds(y + k, modes, stride=tile), :] = out[first : first + modes, lanes * k : lanes * (k + 1)]
            first += modes
        return 0

    lax.fori_loop(0, tile // 4, body, 0)


def x_modes(velocity, table, shares, part=0, parts=1):
    xs, ys, zs = velocity.shape
    modes = table.shape[0] // 2
    tile = 8
    blocks = zs // 128 // parts
    return pl.pallas_call(
        x_kernel,
        grid=(blocks, ys // tile),
        in_specs=[
            pl.BlockSpec((2 * modes, xs), lambda i, k: (0, 0)),
            pl.BlockSpec((xs, 1, tile, 128), lambda i, k: (0, k, 0, part * blocks + i)),
        ],
        out_specs=[pl.BlockSpec((m, 1, tile, 128), lambda i, k: (0, k, 0, i)) for m in shares],
        out_shape=[jax.ShapeDtypeStruct((m, ys // tile, tile, zs // parts), jnp.float32) for m in shares],
        compiler_params=pltpu.CompilerParams(vmem_limit_bytes=VMEM),
        cost_estimate=pl.CostEstimate(flops=6 * modes * xs * ys * zs, bytes_accessed=4 * xs * ys * zs, transcendentals=0),
    )(table, velocity.reshape(xs, ys // tile, tile, zs))


def y_kernel(a_ref, v_ref, *o_refs):
    blocks, _, ys, width = v_ref.shape
    n = blocks * ys
    out = mm3(a_ref[...], v_ref[...].reshape(n, width))
    share = n // len(o_refs)
    for d, o_ref in enumerate(o_refs):
        o_ref[0] = out[d * share : (d + 1) * share]


def y_modes(values, table, parts):
    blocks, planes, ys, zs = values.shape
    n = blocks * ys
    width = zs
    return pl.pallas_call(
        y_kernel,
        grid=(planes, zs // width),
        in_specs=[
            pl.BlockSpec((2 * n, n), lambda i, k: (0, 0)),
            pl.BlockSpec((blocks, 1, ys, width), lambda i, k: (0, i, 0, k)),
        ],
        out_specs=[pl.BlockSpec((1, n // parts, width), lambda i, k: (i, 0, k))] * parts,
        out_shape=[jax.ShapeDtypeStruct((planes, n // parts, zs), jnp.float32)] * parts,
        compiler_params=pltpu.CompilerParams(vmem_limit_bytes=VMEM),
        cost_estimate=pl.CostEstimate(flops=6 * n * n * zs * planes, bytes_accessed=8 * n * zs * planes, transcendentals=0),
    )(table, values)


def table_kernel(cos_ref, sin_ref, plus_ref, minus_ref, high_ref, low_ref):
    inner = plus_ref.shape[0]
    lines = high_ref.shape[0] // inner
    plus, minus = plus_ref[...], minus_ref[...]
    for k in range(lines):
        i = pl.program_id(0) * lines + k
        cos, sin = cos_ref[pl.ds(i, 1), :], sin_ref[pl.ds(i, 1), :]
        high, low = halves(cos * plus + sin * minus)
        high_ref[k * inner : (k + 1) * inner] = high
        low_ref[k * inner : (k + 1) * inner] = low


def wide_table(outer, inner, rank, count):
    width = len(rank)
    unit = 2.0 * jnp.pi / count
    a = unit * (outer[:, None] * rank[None, :] % count).astype(jnp.float32)
    b = unit * (inner[:, None] * rank[None, :] % count).astype(jnp.float32)
    scale = count ** (-0.5)
    cos_b, sin_b = jnp.cos(b), jnp.sin(b)
    lines = pl.BlockSpec((len(outer), width), lambda i: (0, 0))
    whole = pl.BlockSpec((len(inner), width), lambda i: (0, 0))
    block = pl.BlockSpec((4 * len(inner), width), lambda i: (i, 0))
    shape = jax.ShapeDtypeStruct((len(outer) * len(inner), width), jnp.bfloat16)
    return pl.pallas_call(
        table_kernel,
        grid=(len(outer) // 4,),
        in_specs=[lines, lines, whole, whole],
        out_specs=[block, block],
        out_shape=[shape, shape],
        compiler_params=pltpu.CompilerParams(vmem_limit_bytes=VMEM),
        cost_estimate=pl.CostEstimate(flops=10**10, bytes_accessed=2 * count * count, transcendentals=0),
    )(jnp.cos(a) * scale, jnp.sin(a) * scale, cos_b + sin_b, cos_b - sin_b)


def z_kernel(parts, *refs):
    v_refs = refs[:parts]
    he_ref, ho_ref, le_ref, lo_ref, sxy_ref, sz_ref = refs[parts : parts + 6]
    o_ref, high_s, low_s = refs[-3:]
    planes, share, zs = v_refs[0].shape
    rows = planes * share

    @pl.when(pl.program_id(0) == 0)
    def _():
        for p in range(parts // 2):
            near, far = v_refs[p][...].reshape(rows, zs), v_refs[p + parts // 2][...].reshape(rows, zs)
            for k, mixed in enumerate((near + far, near - far)):
                high, low = halves(mixed)
                high_s[k, :, p * zs : (p + 1) * zs] = high
                low_s[k, :, p * zs : (p + 1) * zs] = low

    both = []
    for k, (h_ref, l_ref) in enumerate(((he_ref, le_ref), (ho_ref, lo_ref))):
        high, hr = high_s[k], h_ref[...]
        both.append(mm(high, hr) + mm(low_s[k], hr) + mm(high, l_ref[...]))
    even, odd = both
    sxy = sxy_ref[...]
    lane = lax.broadcasted_iota(jnp.int32, (rows, 128), 1)
    for c in range(0, o_ref.shape[2], 128):
        g = c // 256 * 128
        pick = lane // 2 + c // 128 % 2 * 64
        here = [jnp.take_along_axis(t[:, g : g + 128], pick, axis=1, mode="promise_in_bounds") for t in (even, odd)]
        out = jnp.where(lane % 2 == 0, *here)
        step = 0.2 * (sxy + sz_ref[:, c : c + 128])
        done = out * ((1.0 - step) / (1.0 + step))
        o_ref[:, :, c : c + 128] = done.reshape(planes, share, 128)


def z_modes(values, tables, sxy, symbol_z, start, total, previous):
    parts = len(values)
    planes, share, zs = values[0].shape
    n = parts * zs
    rows = planes * share
    cols = Z_COLS
    steps = n // cols
    high, low = tables
    table_specs = [
        pl.BlockSpec((n // 2, cols // 2), lambda i: (0, i)),
        pl.BlockSpec((n // 2, cols // 2), lambda i: (0, steps + i)),
    ]
    operands = [*values, high, high, low, low, sxy, symbol_z]
    in_specs = [pl.BlockSpec((planes, share, zs), lambda i: (0, 0, 0))] * parts + table_specs * 2 + [
        pl.BlockSpec((pl.Element(rows), pl.Element(128)), lambda i: (start * share, 0)),
        pl.BlockSpec((1, cols), lambda i: (0, i)),
    ]
    aliases = {}
    if previous is not None:
        aliases = {len(operands): 0}
        operands.append(previous)
        in_specs.append(pl.BlockSpec(memory_space=pl.ANY))
    return pl.pallas_call(
        functools.partial(z_kernel, parts),
        grid=(steps,),
        in_specs=in_specs,
        out_specs=pl.BlockSpec(
            (pl.Element(planes), pl.Element(share), pl.Element(cols)), lambda i: (start, 0, i * cols)
        ),
        out_shape=jax.ShapeDtypeStruct((total, share, n), jnp.float32),
        scratch_shapes=[pltpu.VMEM((2, rows, n // 2), jnp.bfloat16)] * 2,
        input_output_aliases=aliases,
        compiler_params=pltpu.CompilerParams(vmem_limit_bytes=VMEM),
        cost_estimate=pl.CostEstimate(flops=3 * rows * n * n, bytes_accessed=2 * n * n + 8 * rows * n, transcendentals=0),
    )(*operands)


def local(velocity, symbol_x, symbol_y, symbol_z):
    xs, ys, zs = velocity.shape
    rows, cols = lax.axis_size("row"), lax.axis_size("col")
    me = lax.axis_index("col")
    planes = xs // rows
    all_y, all_z = ys * rows, zs * cols
    share_y = all_y // cols
    part_x = lax.dynamic_slice_in_dim(symbol_x, lax.axis_index("row") * planes, planes)
    part_y = lax.dynamic_slice_in_dim(symbol_y, me * share_y, share_y)
    sxy = jnp.broadcast_to((part_x[:, None] + part_y[None, :])[..., None], (planes, share_y, 128))
    sxy = sxy.reshape(planes * share_y, 128)
    symbol_z = symbol_z.reshape(1, -1)

    y_rank = (jnp.arange(all_y) + me * share_y) % all_y
    y_table = stacked(small_table(y_rank, all_y))
    low_count = 64
    outer = jnp.arange(all_z // 2 // low_count) * low_count
    outer = (me + cols - outer // zs) % cols * zs + outer % zs
    lane = jnp.arange(all_z)
    half = all_z // 2
    z_tables = wide_table(outer, jnp.arange(low_count), lane % half * 2 + lane // half, all_z)

    x_parts = []
    for name, picked in (("x0", CHUNKS[:1]), ("x1", CHUNKS[1:2]), ("x2", CHUNKS[2:])):
        mode = np.concatenate(
            [(np.arange(rows)[:, None] * planes + start + np.arange(size)).reshape(-1) for start, size, _, _ in picked]
        )
        if name == "x2":
            x_table = stacked(small_table(jnp.asarray(mode, jnp.int32), xs))
        elif name == "x0":
            x_table = fixed_table(mode, xs)
        x_parts += x_modes(velocity, x_table, [rows * size for _, size, _, _ in picked], *picked[0][2:])

    waiting = []
    out = None
    for j, (start, size, piece, pieces) in enumerate(CHUNKS):
        part = x_parts[j].reshape(rows, size, ys, zs // pieces)
        part = lax.all_to_all(part, "row", split_axis=0, concat_axis=0, tiled=True)
        part = y_modes(part, y_table, cols)
        part = [part[0]] + [
            lax.ppermute(part[d], "col", [(i, (i + d) % cols) for i in range(cols)]) for d in range(1, cols)
        ]
        waiting.append(part)
        if piece + 1 < pieces:
            continue
        part = [piece[d] for d in range(cols) for piece in waiting]
        waiting = []
        out = z_modes(part, z_tables, sxy, symbol_z, start, planes, out)
    return out


def solution(mesh):
    placed = (P(None, "row", "col"), P(), P(), P())
    return jax.shard_map(local, mesh=mesh, in_specs=placed, out_specs=P("row", "col", None), check_vma=False)
```
